32 devices in a mesh: ctx: 4 (over x, core), section: 8 (over z, y).
Axes of the slice: x: 2, y: 2, z: 4, core: 2. Of those that a mesh axis runs over, the one named last changes fastest.
Arguments:
- query_in: bfloat16 [8, 2, 512, 1024], P('section', None, 'ctx'), may hold values from -200 to 200
- key_in: bfloat16 [8, 2, 512, 128], P('section', None, 'ctx'), may hold values from -5 to 5
- value_in: bfloat16 [8, 2, 512, 128], P('section', None, 'ctx'), may hold values from -24 to 24
- forward_out: bfloat16 [8, 2, 512, 1024], P('section', None, 'ctx'), may hold values from -6 to 6
- log_sum: float32 [8, 2, 8, 512], P('section', None, None, 'ctx'), as said below
- grad_out: bfloat16 [8, 2, 512, 1024], P('section', None, 'ctx'), may hold values from -6 to 6
- block_order: int32 [8], replicated, may hold values from 0 to 7, each once
Outputs:
- grad_query: bfloat16 [8, 2, 512, 1024], P('section', None, 'ctx')
- grad_key: bfloat16 [8, 2, 512, 128], P('section', None, 'ctx')
- grad_value: bfloat16 [8, 2, 512, 128], P('section', None, 'ctx')
The draws below stay inside these ranges and needn't reach their ends.
Inputs may be any that keep to these rules, and one draw needn't show every extreme that they name: For every layer, micro-batch, head and row, log_sum is at least the logarithm of the sum of exp(score) over all key rows of that row's window, masked or not. block_order is a permutation: slot j, rows j * 64 to j * 64 + 63 of the token dimension, holds sequence positions block_order[j] * 64 onward in order.
All inputs are finite; a program needn't handle non-finite values.
Results may differ from the reference program's by a relative error of at most 0.008.
Values may be sent and summed in bfloat16 or wider, within the bound.
A program may use at most 64 MiB of HBM per device.

```python
import jax
import jax.numpy as jnp
from jax import lax

HEADS = 8
HEAD = 128
TOK_DEV = 128
MICRO = 2
WINDOW = 3
SECTIONS = 8
TOKENS = 512
HALF = 64
BLOCKS = 8


def pair_item(key, index):
    item_key = jax.random.fold_in(key, index)
    keys_raw = jnp.clip(jax.random.normal(jax.random.fold_in(item_key, 11), (TOKENS, HEAD), jnp.float32), -5.0, 5.0)
    queries = jnp.clip(jax.random.normal(jax.random.fold_in(item_key, 12), (TOKENS, HEADS, HEAD), jnp.float32), -5.0, 5.0)
    return (queries.reshape(TOKENS, HEADS * HEAD), keys_raw, item_key)


def item_list():
    return jnp.arange(SECTIONS * MICRO, dtype=jnp.int32)


def draw_query_in(key, part):
    items = lax.map(lambda index: pair_item(key, index)[0].astype(jnp.bfloat16), item_list())
    return items.reshape(SECTIONS, MICRO, TOKENS, HEADS * HEAD)


def draw_key_in(key, part):
    items = lax.map(lambda index: pair_item(key, index)[1].astype(jnp.bfloat16), item_list())
    return items.reshape(SECTIONS, MICRO, TOKENS, HEAD)


def log_item(key, index):
    queries, keys_raw, item_key = pair_item(key, index)
    shards = TOKENS // TOK_DEV
    query_low = queries.astype(jnp.bfloat16).astype(jnp.float32).reshape(shards, TOK_DEV, HEADS, HEAD)
    key_low = keys_raw.astype(jnp.bfloat16).astype(jnp.float32).reshape(shards, TOK_DEV, HEAD)
    window_keys = jnp.concatenate([jnp.roll(key_low, offset, axis=0) for offset in range(WINDOW)], axis=1)
    scores = jnp.einsum('cqhd,ckd->chqk', query_low, window_keys, precision=lax.Precision.HIGHEST) / jnp.sqrt(jnp.float32(HEAD))
    top = jnp.max(scores, axis=-1)
    total = jnp.sum(jnp.exp(scores - top[..., None]), axis=-1)
    extra = jnp.exp(jax.random.uniform(jax.random.fold_in(item_key, 14), (shards, HEADS, TOK_DEV), jnp.float32, jnp.log(0.1), jnp.log(2.0)))
    log_rows = top + jnp.log(total + extra)
    return jnp.transpose(log_rows, (1, 0, 2)).reshape(HEADS, TOKENS)


def draw_log_sum(key, part):
    items = lax.map(lambda index: log_item(key, index), item_list())
    return items.reshape(SECTIONS, MICRO, HEADS, TOKENS)


def shard_levels(key, dims, cuts, low, largest):
    def one(axis_at, parts):
        heights = jax.random.uniform(jax.random.fold_in(jax.random.fold_in(key, 6), axis_at), (parts,), jnp.float32, low / len(cuts), largest / len(cuts))
        return jnp.repeat(jnp.exp(heights), dims[axis_at] // parts).reshape((-1,) + (1,) * (len(dims) - axis_at - 1))

    factor_of = one(*cuts[0])
    for cut in cuts[1:]:
        factor_of = factor_of * one(*cut)
    return factor_of


def gaussian(key, shape, deviation, reach, split=(), kind=jnp.bfloat16):
    drawn = deviation * jax.random.normal(key, shape, jnp.float32)
    if split:
        drawn = drawn * shard_levels(key, shape, split, -0.22, 0.18)
    return jnp.clip(drawn, -reach, reach).astype(kind)


def setup_inputs(seed: int = 0) -> dict:
    key_of = jax.random.split(jax.random.key(seed), 8)
    query_in = draw_query_in(jax.random.fold_in(key_of[7], 71), 0)
    key_in = draw_key_in(jax.random.fold_in(key_of[7], 71), 0)
    value_in = gaussian(key_of[2], (SECTIONS, MICRO, TOKENS, HEAD), 4.0, 24.0, ((0, 8), (2, 4)))
    forward_out = gaussian(key_of[3], (SECTIONS, MICRO, TOKENS, HEADS * HEAD), 1.0, 6.0, ((0, 8), (2, 4)))
    log_sum = draw_log_sum(jax.random.fold_in(key_of[7], 71), 0)
    grad_out = gaussian(key_of[5], (SECTIONS, MICRO, TOKENS, HEADS * HEAD), 1.0, 6.0, ((0, 8), (2, 4)))
    block_order = jax.random.permutation(key_of[6], BLOCKS).astype(jnp.int32)
    return {"query_in": query_in, "key_in": key_in, "value_in": value_in, "forward_out": forward_out, "log_sum": log_sum, "grad_out": grad_out, "block_order": block_order}


def place_rows(block_order, length, half_rows):
    row_ids = jnp.arange(length, dtype=jnp.int32)
    slot_ids = row_ids // half_rows
    lookup = (slot_ids[:, None] == jnp.arange(block_order.shape[0], dtype=jnp.int32)[None, :]).astype(jnp.int32)
    return lax.optimization_barrier(jnp.sum(lookup * block_order[None, :], axis=1)) * half_rows + row_ids % half_rows

def round_keep(values_in):
    return lax.optimization_barrier(values_in.astype(jnp.bfloat16)).astype(jnp.float32)

def layer_backward(query_rows, key_rows, value_rows, saved_out, saved_log, upstream, places):
    shards = TOKENS // TOK_DEV
    factor = 1.0 / jnp.sqrt(jnp.float32(HEAD))
    query_heads = query_rows.reshape(shards, TOK_DEV, HEADS, HEAD).astype(jnp.float32)
    grad_heads = upstream.reshape(shards, TOK_DEV, HEADS, HEAD).astype(jnp.float32)
    out_heads = saved_out.reshape(shards, TOK_DEV, HEADS, HEAD).astype(jnp.float32)
    row_dot = jnp.transpose(lax.optimization_barrier(jnp.sum(grad_heads * out_heads, axis=-1)), (0, 2, 1))
    log_rows = jnp.transpose(saved_log.reshape(HEADS, shards, TOK_DEV), (1, 0, 2))
    key_float = key_rows.reshape(shards, TOK_DEV, HEAD).astype(jnp.float32)
    value_float = value_rows.reshape(shards, TOK_DEV, HEAD).astype(jnp.float32)
    place_shards = places.reshape(shards, TOK_DEV)
    grad_query = jnp.zeros((shards, TOK_DEV, HEADS, HEAD), jnp.float32)
    grad_key = jnp.zeros((shards, TOK_DEV, HEAD), jnp.float32)
    grad_value = jnp.zeros((shards, TOK_DEV, HEAD), jnp.float32)
    for offset in range(WINDOW):
        key_near = jnp.roll(key_float, offset, axis=0)
        value_near = jnp.roll(value_float, offset, axis=0)
        place_near = jnp.roll(place_shards, offset, axis=0)
        scores = jnp.einsum('cqhd,ckd->chqk', query_heads, key_near) * factor
        visible = place_shards[:, :, None] >= place_near[:, None, :]
        probs = jnp.where(visible[:, None], jnp.exp(scores - log_rows[..., None]), 0.0)
        grad_probs = jnp.einsum('cqhd,ckd->chqk', grad_heads, value_near)
        grad_scores = round_keep(probs * (grad_probs - row_dot[..., None]))
        probs_low = round_keep(probs)
        grad_query = grad_query + jnp.einsum('chqk,ckd->cqhd', grad_scores, key_near) * factor
        key_terms = jnp.einsum('chqk,cqhd->ckd', grad_scores, query_heads) * factor
        value_terms = jnp.einsum('chqk,cqhd->ckd', probs_low, grad_heads)
        grad_key = grad_key + jnp.roll(key_terms, -offset, axis=0)
        grad_value = grad_value + jnp.roll(value_terms, -offset, axis=0)
    return (grad_query.reshape(TOKENS, HEADS * HEAD).astype(jnp.bfloat16), grad_key.reshape(TOKENS, HEAD).astype(jnp.bfloat16), grad_value.reshape(TOKENS, HEAD).astype(jnp.bfloat16))

def reference(query_in, key_in, value_in, forward_out, log_sum, grad_out, block_order):
    places = place_rows(block_order, TOKENS, HALF)

    def run_layer(items):
        return layer_backward(items[0], items[1], items[2], items[3], items[4], items[5], places)
    first = lax.map(run_layer, (query_in[:, 0], key_in[:, 0], value_in[:, 0], forward_out[:, 0], log_sum[:, 0], grad_out[:, 0]))
    passed = jnp.concatenate([first[0][1:], jnp.zeros_like(first[0][:1])], axis=0)
    upstream = (grad_out[:, 1].astype(jnp.float32) + passed.astype(jnp.float32)).astype(jnp.bfloat16)
    second = lax.map(run_layer, (query_in[:, 1], key_in[:, 1], value_in[:, 1], forward_out[:, 1], log_sum[:, 1], upstream))
    grad_query = jnp.stack([first[0], second[0]], axis=1)
    grad_key = jnp.stack([first[1], second[1]], axis=1)
    grad_value = jnp.stack([first[2], second[2]], axis=1)
    return (grad_query, grad_key, grad_value)
```

```python
import functools
import math

import jax
import jax.numpy as jnp
from jax import lax
from jax.experimental import pallas as pl
from jax.experimental.pallas import tpu as pltpu
from jax.sharding import PartitionSpec as P

WINDOW = 3
LOG2E = math.log2(math.e)
HIDE = -1e30


def dot(a, b, dims):
    return lax.dot_general(a, b, (dims, ((), ())), preferred_element_type=jnp.float32)


def kernel(
    members, sections, blocks,
    order_ref, q_hbm, k_hbm, v_hbm, fo_hbm, go_hbm, log_hbm,
    dq_hbm, dk_hbm, dv_hbm,
    q, fo, go, logs, kv, bias, dq, passed, own, part, back, kv_out,
    q_sem, fo_sem, go_sem, log_sem, kv_sem,
    kv_send, kv_recv, part_send, part_recv, hop_send, hop_recv, dq_sem, kv_out_sem,
):
    micro, rows, width = q.shape
    head = kv.shape[-1]
    chunks, _, wide = passed.shape
    group = wide // head
    span = group * rows
    factor = 1.0 / math.sqrt(head)
    me = lax.axis_index("ctx")
    sec = lax.axis_index("section")
    peer = lambda offset: {"ctx": lax.rem(me + offset + members, members)}
    below = {"section": jnp.maximum(sec - 1, 0)}
    above = {"section": jnp.minimum(sec + 1, sections - 1)}
    has_below = sec > 0
    has_above = sec < sections - 1

    kv_loads, loads = [], []
    for m in range(micro):
        for which, source in enumerate((k_hbm, v_hbm)):
            copy = pltpu.make_async_copy(source.at[0, m], kv.at[m, 0, which], kv_sem.at[m, which])
            copy.start()
            kv_loads.append(copy)
    for m in range(micro):
        now = [
            pltpu.make_async_copy(log_hbm.at[0, m], logs.at[m], log_sem.at[m]),
            pltpu.make_async_copy(q_hbm.at[0, m], q.at[m], q_sem.at[m]),
            pltpu.make_async_copy(go_hbm.at[0, m], go.at[m], go_sem.at[m]),
            pltpu.make_async_copy(fo_hbm.at[0, m], fo.at[m], fo_sem.at[m]),
        ]
        for copy in now:
            copy.start()
        loads.append(now)

    barrier = pltpu.get_barrier_semaphore()
    near = sorted({o % members for o in range(1 - WINDOW, WINDOW)} - {0})
    for o in near:
        pl.semaphore_signal(barrier, inc=1, device_id=peer(o), device_id_type=pl.DeviceIdType.MESH)

    @pl.when(has_below)
    def _():
        pl.semaphore_signal(barrier, inc=1, device_id=below, device_id_type=pl.DeviceIdType.MESH)

    @pl.when(has_above)
    def _():
        pl.semaphore_signal(barrier, inc=1, device_id=above, device_id_type=pl.DeviceIdType.MESH)

    half = members * rows // blocks
    per = rows // half
    lane = lax.broadcasted_iota(jnp.int32, (half, rows), 1)
    down = lax.broadcasted_iota(jnp.int32, (half, rows), 0)
    q_place = lax.rem(lane, half)
    for b in range(per):
        base = order_ref[me * per + b] * half
        q_place = q_place + jnp.where(lane // half == b, base, 0)
    for o in range(WINDOW):
        source = lax.rem(me - o + members, members)
        for b in range(per):
            k_place = down + order_ref[source * per + b] * half
            tile = jnp.where(k_place <= q_place, 0.0, HIDE)
            for g in range(group):
                bias[pl.ds(o * rows + b * half, half), pl.ds(g * rows, rows)] = tile

    @pl.when(jnp.logical_not(has_above))
    def _():
        passed[...] = jnp.zeros_like(passed)

    pl.semaphore_wait(barrier, len(near) + has_below.astype(jnp.int32) + has_above.astype(jnp.int32))

    def send_kv(m):
        copies = []
        for o in range(WINDOW - 1, 0, -1):
            copy = pltpu.make_async_remote_copy(
                src_ref=kv.at[m, 0], dst_ref=kv.at[m, o],
                send_sem=kv_send.at[m, o - 1], recv_sem=kv_recv.at[m, o - 1],
                device_id=peer(o), device_id_type=pl.DeviceIdType.MESH,
            )
            copy.start()
            copies.append(copy)
        return copies

    kv_loads[0].wait()
    kv_loads[1].wait()
    kv_copies = [send_kv(0)]

    ones = jnp.ones((8, head), jnp.bfloat16)
    hops, dq_outs, part_copies = [], [], []

    def split(block):
        return jnp.concatenate([block[:, g * head:(g + 1) * head] for g in range(group)], axis=0)

    for m in range(micro):
        for copy in loads[m]:
            copy.wait()
        for copy in kv_copies[m]:
            copy.wait_recv()
        if m == 0:
            for copy in kv_loads[2:]:
                copy.wait()
            for later in range(1, micro):
                kv_copies.append(send_kv(later))
        keys = jnp.concatenate([kv[m, o, 0] for o in range(WINDOW)], axis=0)
        values = jnp.concatenate([kv[m, o, 1] for o in range(WINDOW)], axis=0)
        dk_total = dv_total = None
        for c in range(chunks):
            cols = pl.ds(c * wide, wide)
            queries = split(q[m, :, cols])
            upstream = go[m, :, cols]
            if m > 0:
                if m == 1:
                    @pl.when(has_above)
                    def _(c=c):
                        hop(c).wait_recv()
                upstream = (
                    upstream.astype(jnp.float32) + passed[c].astype(jnp.float32)
                ).astype(jnp.bfloat16)
            upstream = split(upstream)
            product = upstream.astype(jnp.float32) * split(fo[m, :, cols]).astype(jnp.float32)
            high = product.astype(jnp.bfloat16)
            low = (product - high.astype(jnp.float32)).astype(jnp.bfloat16)
            row_dot = (dot(ones, high, ((1,), (1,))) + dot(ones, low, ((1,), (1,))))[0:1]
            log_row = jnp.concatenate(
                [logs[m, pl.ds(c * group + g, 1), :] for g in range(group)], axis=1
            ) * LOG2E
            scores = dot(keys, queries, ((1,), (1,)))
            probs = jnp.exp2(scores * (factor * LOG2E) - log_row + bias[...])
            grad_probs = dot(values, upstream, ((1,), (1,)))
            grad_scores = (probs * (grad_probs - row_dot)).astype(jnp.bfloat16)
            grad_query = dot(grad_scores, keys, ((0,), (0,))) * factor
            for g in range(group):
                dq[m, c, :, pl.ds(g * head, head)] = grad_query[g * rows:(g + 1) * rows].astype(jnp.bfloat16)
            if m == 0:
                def hop(c):
                    return pltpu.make_async_remote_copy(
                        src_ref=dq.at[0, c], dst_ref=passed.at[c],
                        send_sem=hop_send.at[c], recv_sem=hop_recv.at[c],
                        device_id=below, device_id_type=pl.DeviceIdType.MESH,
                    )

                @pl.when(has_below)
                def _(c=c):
                    hop(c).start()
            copy = pltpu.make_async_copy(dq.at[m, c], dq_hbm.at[0, m, :, cols], dq_sem.at[m, c])
            copy.start()
            dq_outs.append(copy)
            dk = dot(grad_scores, queries, ((1,), (0,)))
            dv = dot(probs.astype(jnp.bfloat16), upstream, ((1,), (0,)))
            dk_total = dk if dk_total is None else dk_total + dk
            dv_total = dv if dv_total is None else dv_total + dv
        dk_total = dk_total * factor
        for o in range(WINDOW - 1, 0, -1):
            for which, total in enumerate((dk_total, dv_total)):
                part[m, o - 1, which] = total[o * rows:(o + 1) * rows].astype(jnp.bfloat16)
            copy = pltpu.make_async_remote_copy(
                src_ref=part.at[m, o - 1], dst_ref=back.at[m, o - 1],
                send_sem=part_send.at[m, o - 1], recv_sem=part_recv.at[m, o - 1],
                device_id=peer(-o), device_id_type=pl.DeviceIdType.MESH,
            )
            copy.start()
            part_copies.append((m, o, copy))
        own[m, 0] = dk_total[:rows]
        own[m, 1] = dv_total[:rows]

    kv_outs = []
    for m in range(micro):
        for at, o, copy in part_copies:
            if at == m:
                copy.wait_recv()
        for which, target in enumerate((dk_hbm, dv_hbm)):
            total = own[m, which]
            for o in range(1, WINDOW):
                total = total + back[m, o - 1, which].astype(jnp.float32)
            kv_out[m, which] = total.astype(jnp.bfloat16)
            copy = pltpu.make_async_copy(kv_out.at[m, which], target.at[0, m], kv_out_sem.at[m, which])
            copy.start()
            kv_outs.append(copy)
    for copies in kv_copies:
        for copy in copies:
            copy.wait_send()
    for _, _, copy in part_copies:
        copy.wait_send()

    @pl.when(has_below)
    def _():
        for c in range(chunks):
            hop(c).wait_send()

    for copy in dq_outs + kv_outs:
        copy.wait()


def solution(mesh):
    members = mesh.shape["ctx"]
    sections = mesh.shape["section"]
    in_specs = (
        P("section", None, "ctx", None),
        P("section", None, "ctx", None),
        P("section", None, "ctx", None),
        P("section", None, "ctx", None),
        P("section", None, None, "ctx"),
        P("section", None, "ctx", None),
        P(),
    )
    out_specs = (
        P("section", None, "ctx", None),
        P("section", None, "ctx", None),
        P("section", None, "ctx", None),
    )

    def shards(query_in, key_in, value_in, forward_out, log_sum, grad_out, block_order):
        _, micro, rows, width = query_in.shape
        head = key_in.shape[3]
        heads = width // head
        group = 2 if heads % 2 == 0 else 1
        chunks = heads // group
        wide = group * head
        low, full = jnp.bfloat16, jnp.float32
        dma = pltpu.SemaphoreType.DMA
        others = WINDOW - 1
        return pl.pallas_call(
            functools.partial(kernel, members, sections, block_order.shape[0]),
            out_shape=(
                jax.ShapeDtypeStruct(query_in.shape, low),
                jax.ShapeDtypeStruct(key_in.shape, low),
                jax.ShapeDtypeStruct(value_in.shape, low),
            ),
            in_specs=[pl.BlockSpec(memory_space=pltpu.SMEM)]
            + [pl.BlockSpec(memory_space=pl.ANY)] * 6,
            out_specs=[pl.BlockSpec(memory_space=pl.ANY)] * 3,
            scratch_shapes=[
                pltpu.VMEM((micro, rows, width), low),
                pltpu.VMEM((micro, rows, width), low),
                pltpu.VMEM((micro, rows, width), low),
                pltpu.VMEM((micro, heads, rows), full),
                pltpu.VMEM((micro, WINDOW, 2, rows, head), low),
                pltpu.VMEM((WINDOW * rows, group * rows), full),
                pltpu.VMEM((micro, chunks, rows, wide), low),
                pltpu.VMEM((chunks, rows, wide), low),
                pltpu.VMEM((micro, 2, rows, head), full),
                pltpu.VMEM((micro, others, 2, rows, head), low),
                pltpu.VMEM((micro, others, 2, rows, head), low),
                pltpu.VMEM((micro, 2, rows, head), low),
                dma((micro,)), dma((micro,)), dma((micro,)), dma((micro,)), dma((micro, 2)),
                dma((micro, others)), dma((micro, others)),
                dma((micro, others)), dma((micro, others)),
                dma((chunks,)), dma((chunks,)),
                dma((micro, chunks)), dma((micro, 2)),
            ],
            compiler_params=pltpu.CompilerParams(collective_id=0, has_side_effects=True),
        )(block_order, query_in, key_in, value_in, forward_out, grad_out, log_sum)

    return jax.shard_map(shards, mesh=mesh, in_specs=in_specs, out_specs=out_specs, check_vma=False)
```

```python
import functools
import math

import jax
import jax.numpy as jnp
from jax import lax
from jax.experimental import pallas as pl
from jax.experimental.pallas import tpu as pltpu
from jax.sharding import PartitionSpec as P

WINDOW = 3
LOG2E = math.log2(math.e)
HIDE = -1e30


def dot(a, b, dims):
    return lax.dot_general(a, b, (dims, ((), ())), preferred_element_type=jnp.float32)


def kernel(
    members, sections, blocks,
    order_ref, q_hbm, k_hbm, v_hbm, fo_hbm, go_hbm, log_hbm,
    dq, kv_out,
    q, fo, go, logs, kv, bias, passed, own, part, back,
    q_sem, fo_sem, go_sem, log_sem, kv_sem,
    kv_send, kv_recv, part_send, part_recv, hop_send, hop_recv,
):
    micro, rows, width = q.shape
    head = kv.shape[-1]
    chunks, _, wide = passed.shape
    group = wide // head
    span = group * rows
    factor = 1.0 / math.sqrt(head)
    me = lax.axis_index("ctx")
    sec = lax.axis_index("section")
    peer = lambda offset: {"ctx": lax.rem(me + offset + members, members)}
    below = {"section": jnp.maximum(sec - 1, 0)}
    above = {"section": jnp.minimum(sec + 1, sections - 1)}
    has_below = sec > 0
    has_above = sec < sections - 1

    kv_loads, loads = [], []
    for m in range(micro):
        for which, source in enumerate((k_hbm, v_hbm)):
            copy = pltpu.make_async_copy(source.at[0, m], kv.at[m, 0, which], kv_sem.at[m, which])
            copy.start()
            kv_loads.append(copy)
    for m in range(micro):
        now = [
            pltpu.make_async_copy(log_hbm.at[0, m], logs.at[m], log_sem.at[m]),
            pltpu.make_async_copy(q_hbm.at[0, m], q.at[m], q_sem.at[m]),
            pltpu.make_async_copy(go_hbm.at[0, m], go.at[m], go_sem.at[m]),
            pltpu.make_async_copy(fo_hbm.at[0, m], fo.at[m], fo_sem.at[m]),
        ]
        for copy in now:
            copy.start()
        loads.append(now)

    barrier = pltpu.get_barrier_semaphore()
    near = sorted({o % members for o in range(1 - WINDOW, WINDOW)} - {0})
    for o in near:
        pl.semaphore_signal(barrier, inc=1, device_id=peer(o), device_id_type=pl.DeviceIdType.MESH)

    @pl.when(has_below)
    def _():
        pl.semaphore_signal(barrier, inc=1, device_id=below, device_id_type=pl.DeviceIdType.MESH)

    @pl.when(has_above)
    def _():
        pl.semaphore_signal(barrier, inc=1, device_id=above, device_id_type=pl.DeviceIdType.MESH)

    half = members * rows // blocks
    per = rows // half
    lane = lax.broadcasted_iota(jnp.int32, (half, rows), 1)
    down = lax.broadcasted_iota(jnp.int32, (half, rows), 0)
    q_place = lax.rem(lane, half)
    for b in range(per):
        base = order_ref[me * per + b] * half
        q_place = q_place + jnp.where(lane // half == b, base, 0)
    for o in range(WINDOW):
        source = lax.rem(me - o + members, members)
        for b in range(per):
            k_place = down + order_ref[source * per + b] * half
            tile = jnp.where(k_place <= q_place, 0.0, HIDE)
            for g in range(group):
                bias[pl.ds(o * rows + b * half, half), pl.ds(g * rows, rows)] = tile

    @pl.when(jnp.logical_not(has_above))
    def _():
        passed[...] = jnp.zeros_like(passed)

    pl.semaphore_wait(barrier, len(near) + has_below.astype(jnp.int32) + has_above.astype(jnp.int32))

    def send_kv(m):
        copies = []
        for o in range(WINDOW - 1, 0, -1):
            copy = pltpu.make_async_remote_copy(
                src_ref=kv.at[m, 0], dst_ref=kv.at[m, o],
                send_sem=kv_send.at[m, o - 1], recv_sem=kv_recv.at[m, o - 1],
                device_id=peer(o), device_id_type=pl.DeviceIdType.MESH,
            )
            copy.start()
            copies.append(copy)
        return copies

    kv_loads[0].wait()
    kv_loads[1].wait()
    kv_copies = [send_kv(0)]

    ones = jnp.ones((8, head), jnp.bfloat16)
    part_copies = []

    def split(block):
        return jnp.concatenate([block[:, g * head:(g + 1) * head] for g in range(group)], axis=0)

    for m in range(micro):
        for copy in loads[m]:
            copy.wait()
        for copy in kv_copies[m]:
            copy.wait_recv()
        if m == 0:
            for copy in kv_loads[2:]:
                copy.wait()
            for later in range(1, micro):
                kv_copies.append(send_kv(later))
        keys = jnp.concatenate([kv[m, o, 0] for o in range(WINDOW)], axis=0)
        values = jnp.concatenate([kv[m, o, 1] for o in range(WINDOW)], axis=0)
        dk_total = dv_total = None
        for c in range(chunks):
            cols = pl.ds(c * wide, wide)
            queries = split(q[m, :, cols])
            upstream = go[m, :, cols]
            if m > 0:
                if m == 1:
                    @pl.when(has_above)
                    def _(c=c):
                        hop(c).wait_recv()
                upstream = (
                    upstream.astype(jnp.float32) + passed[c].astype(jnp.float32)
                ).astype(jnp.bfloat16)
            upstream = split(upstream)
            product = upstream.astype(jnp.float32) * split(fo[m, :, cols]).astype(jnp.float32)
            high = product.astype(jnp.bfloat16)
            low = (product - high.astype(jnp.float32)).astype(jnp.bfloat16)
            row_dot = (dot(ones, high, ((1,), (1,))) + dot(ones, low, ((1,), (1,))))[0:1]
            log_row = jnp.concatenate(
                [logs[m, pl.ds(c * group + g, 1), :] for g in range(group)], axis=1
            ) * LOG2E
            scores = dot(keys, queries, ((1,), (1,)))
            probs = jnp.exp2(scores * (factor * LOG2E) - log_row + bias[...])
            grad_probs = dot(values, upstream, ((1,), (1,)))
            grad_scores = (probs * (grad_probs - row_dot)).astype(jnp.bfloat16)
            grad_query = dot(grad_scores, keys, ((0,), (0,))) * factor
            for g in range(group):
                dq[m, c, :, pl.ds(g * head, head)] = grad_query[g * rows:(g + 1) * rows].astype(jnp.bfloat16)
            if m == 0:
                def hop(c):
                    return pltpu.make_async_remote_copy(
                        src_ref=dq.at[0, c], dst_ref=passed.at[c],
                        send_sem=hop_send.at[c], recv_sem=hop_recv.at[c],
                        device_id=below, device_id_type=pl.DeviceIdType.MESH,
                    )

                @pl.when(has_below)
                def _(c=c):
                    hop(c).start()
            dk = dot(grad_scores, queries, ((1,), (0,)))
            dv = dot(probs.astype(jnp.bfloat16), upstream, ((1,), (0,)))
            dk_total = dk if dk_total is None else dk_total + dk
            dv_total = dv if dv_total is None else dv_total + dv
        dk_total = dk_total * factor
        for o in range(WINDOW - 1, 0, -1):
            for which, total in enumerate((dk_total, dv_total)):
                part[m, o - 1, which] = total[o * rows:(o + 1) * rows].astype(jnp.bfloat16)
            copy = pltpu.make_async_remote_copy(
                src_ref=part.at[m, o - 1], dst_ref=back.at[m, o - 1],
                send_sem=part_send.at[m, o - 1], recv_sem=part_recv.at[m, o - 1],
                device_id=peer(-o), device_id_type=pl.DeviceIdType.MESH,
            )
            copy.start()
            part_copies.append((m, o, copy))
        own[m, 0] = dk_total[:rows]
        own[m, 1] = dv_total[:rows]

    for m in range(micro):
        for at, o, copy in part_copies:
            if at == m:
                copy.wait_recv()
        for which in range(2):
            total = own[m, which]
            for o in range(1, WINDOW):
                total = total + back[m, o - 1, which].astype(jnp.float32)
            kv_out[m, which] = total.astype(jnp.bfloat16)
    for copies in kv_copies:
        for copy in copies:
            copy.wait_send()
    for _, _, copy in part_copies:
        copy.wait_send()

    @pl.when(has_below)
    def _():
        for c in range(chunks):
            hop(c).wait_send()


def writer(dq, kv_out, dq_hbm, dk_hbm, dv_hbm, dq_sem, kv_sem):
    micro, chunks, _, wide = dq.shape
    copies = []
    for m in range(micro):
        for c in range(chunks):
            copies.append(pltpu.make_async_copy(
                dq.at[m, c], dq_hbm.at[0, m, :, pl.ds(c * wide, wide)], dq_sem.at[m, c]
            ))
        for which, target in enumerate((dk_hbm, dv_hbm)):
            copies.append(pltpu.make_async_copy(
                kv_out.at[m, which], target.at[0, m], kv_sem.at[m, which]
            ))
    for copy in copies:
        copy.start()
    for copy in copies:
        copy.wait()


def solution(mesh):
    members = mesh.shape["ctx"]
    sections = mesh.shape["section"]
    in_specs = (
        P("section", None, "ctx", None),
        P("section", None, "ctx", None),
        P("section", None, "ctx", None),
        P("section", None, "ctx", None),
        P("section", None, None, "ctx"),
        P("section", None, "ctx", None),
        P(),
    )
    out_specs = (
        P("section", None, "ctx", None),
        P("section", None, "ctx", None),
        P("section", None, "ctx", None),
    )

    def shards(query_in, key_in, value_in, forward_out, log_sum, grad_out, block_order):
        _, micro, rows, width = query_in.shape
        head = key_in.shape[3]
        heads = width // head
        group = 2 if heads % 2 == 0 else 1
        chunks = heads // group
        wide = group * head
        low, full = jnp.bfloat16, jnp.float32
        dma = pltpu.SemaphoreType.DMA
        others = WINDOW - 1
        dq, kv_out = pl.pallas_call(
            functools.partial(kernel, members, sections, block_order.shape[0]),
            out_shape=(
                pltpu.VMEM((micro, chunks, rows, wide), low),
                pltpu.VMEM((micro, 2, rows, head), low),
            ),
            in_specs=[pl.BlockSpec(memory_space=pltpu.SMEM)]
            + [pl.BlockSpec(memory_space=pl.ANY)] * 6,
            out_specs=[pl.BlockSpec(memory_space=pltpu.VMEM)] * 2,
            scratch_shapes=[
                pltpu.VMEM((micro, rows, width), low),
                pltpu.VMEM((micro, rows, width), low),
                pltpu.VMEM((micro, rows, width), low),
                pltpu.VMEM((micro, heads, rows), full),
                pltpu.VMEM((micro, WINDOW, 2, rows, head), low),
                pltpu.VMEM((WINDOW * rows, group * rows), full),
                pltpu.VMEM((chunks, rows, wide), low),
                pltpu.VMEM((micro, 2, rows, head), full),
                pltpu.VMEM((micro, others, 2, rows, head), low),
                pltpu.VMEM((micro, others, 2, rows, head), low),
                dma((micro,)), dma((micro,)), dma((micro,)), dma((micro,)), dma((micro, 2)),
                dma((micro, others)), dma((micro, others)),
                dma((micro, others)), dma((micro, others)),
                dma((chunks,)), dma((chunks,)),
            ],
            compiler_params=pltpu.CompilerParams(collective_id=0, has_side_effects=True),
        )(block_order, query_in, key_in, value_in, forward_out, grad_out, log_sum)
        return pl.pallas_call(
            writer,
            out_shape=(
                jax.ShapeDtypeStruct(query_in.shape, low),
                jax.ShapeDtypeStruct(key_in.shape, low),
                jax.ShapeDtypeStruct(value_in.shape, low),
            ),
            in_specs=[pl.BlockSpec(memory_space=pltpu.VMEM)] * 2,
            out_specs=[pl.BlockSpec(memory_space=pl.ANY)] * 3,
            scratch_shapes=[dma((micro, chunks)), dma((micro, 2))],
        )(*(pltpu.with_memory_space_constraint(x, pltpu.VMEM) for x in (dq, kv_out)))

    return jax.shard_map(shards, mesh=mesh, in_specs=in_specs, out_specs=out_specs, check_vma=False)
```
